16 devices in a mesh: data: 4 (over z, y), tp: 4 (over x, core).
Axes of the slice: x: 2, y: 2, z: 2, core: 2. Of those that a mesh axis runs over, the one named last changes fastest.
Arguments:
- attn_out: bfloat16 [1024, 8192], P('data', 'tp'), parts along dimension 0
- w_out: bfloat16 [8192, 8192], P('tp')
- residual: bfloat16 [1024, 8192], P('data', 'tp'), parts along dimension 0
- norm_gain: float32 [8192], P('tp')
Outputs:
- output 1: bfloat16 [1024, 8192], P('data', 'tp'), parts along dimension 0
- output 2: bfloat16 [1024, 8192], P('data', 'tp'), parts along dimension 0
There are 4 independent parts. The reference program is written for one: setup_inputs(seed, part) draws one part's arguments, and reference() takes and returns one part's arrays. A program takes and returns all parts, laid end to end along the dimension named above; an argument that names none is the same for every part.
All inputs are finite; a program needn't handle non-finite values.
Results may differ from the reference program's by a relative error of at most 0.00644529.
Values are sent between devices in bfloat16 or wider.
A program may use at most 1 GiB of HBM per device.

```python
import jax
import jax.numpy as jnp
from jax import lax

D_MODEL = 8192
N_HEADS = 32
HEAD_DIM = 256
TOKENS = 256
EPS = 1e-5


def setup_inputs(seed: int = 0, part: int = 0) -> dict:
    proj_width = N_HEADS * HEAD_DIM
    part_key = jax.random.fold_in(jax.random.key(seed), part)
    key_attn, key_resid = jax.random.split(part_key, 2)
    key_weight, key_gain = jax.random.split(jax.random.key(seed + 1), 2)
    attn_out = jax.random.normal(key_attn, (TOKENS, proj_width), jnp.float32).astype(jnp.bfloat16)
    weight_vals = jax.random.normal(key_weight, (proj_width, D_MODEL), jnp.float32) * proj_width ** -0.5
    w_out = weight_vals.astype(jnp.bfloat16)
    residual = jax.random.normal(key_resid, (TOKENS, D_MODEL), jnp.float32).astype(jnp.bfloat16)
    norm_gain = jax.random.uniform(key_gain, (D_MODEL,), jnp.float32, 0.5, 1.5)
    return {"attn_out": attn_out, "w_out": w_out, "residual": residual, "norm_gain": norm_gain}


def reference(attn_out, w_out, residual, norm_gain):
    projected = jnp.dot(attn_out, w_out, preferred_element_type=jnp.float32)
    hidden = residual.astype(jnp.float32) + projected
    mean_sq = jnp.mean(hidden * hidden, axis=-1, keepdims=True)
    normed = hidden * lax.rsqrt(mean_sq + EPS) * norm_gain
    return (hidden.astype(jnp.bfloat16), normed.astype(jnp.bfloat16))
```

```python
import functools

import jax
import jax.numpy as jnp
from jax import lax
from jax.experimental import pallas as pl
from jax.experimental.pallas import tpu as pltpu
from jax.sharding import PartitionSpec as P

EPS = 1e-5
CN = 256
RB = 128
DEPTH = 6
LANES = 128
MESH = pl.DeviceIdType.MESH


def kernel(n_tp, a_hbm, w_hbm, r_hbm, g_hbm, hid_ref, nrm_ref,
           a, w, res, gain, sbuf, pbuf, own, rbuf, sq, st_out, st_in,
           a_sem, w_sem, r_sem, g_sem, ss_sem, sp_sem, rr_sem, rp_sem, sst_sem, rst_sem):
    rows, d_local = hid_ref.shape
    d_model = d_local * n_tp
    nch = d_local // CN
    nrb = rows // RB
    half = 2 * nch
    total = 4 * nch

    me = lax.axis_index("tp")
    chip = me // 2
    core = me % 2
    partner = chip * 2 + (1 - core)
    far = (1 - chip) * 2

    def dev(t):
        return {"tp": t}

    def owner_chunk(i):
        if isinstance(i, int):
            if i < half:
                return far + i % 2, i // 2
            if i < half + nch:
                return partner, i - half
            return me, i - half - nch
        is_far = jnp.int32(i < half)
        is_part = jnp.int32(i < half + nch) - is_far
        is_own = 1 - is_far - is_part
        o = is_far * (far + i % 2) + is_part * partner + is_own * me
        c = is_far * (i // 2) + is_part * (i - half) + is_own * (i - half - nch)
        return o, c

    def w_copy(i):
        o, c = owner_chunk(i)
        col = pl.multiple_of(o * d_local + c * CN, CN)
        return pltpu.make_async_copy(w_hbm.at[:, pl.ds(col, CN)], w.at[i], w_sem.at[i])

    a_copy = pltpu.make_async_copy(a_hbm, a, a_sem)
    a_copy.start()
    for i in range(DEPTH):
        w_copy(i).start()
    r_copy = pltpu.make_async_copy(r_hbm, res, r_sem)
    r_copy.start()
    g_copy = pltpu.make_async_copy(g_hbm, gain, g_sem)
    g_copy.start()

    barrier = pltpu.get_barrier_semaphore()
    for k in range(1, n_tp):
        pl.semaphore_signal(barrier, inc=1, device_id=dev((me + k) % n_tp), device_id_type=MESH)

    def product(i):
        @pl.when(i + DEPTH < total)
        def _():
            w_copy(i + DEPTH).start()

        w_copy(i).wait()
        return jnp.dot(a[...], w[i], preferred_element_type=jnp.float32)

    def far_send(i, b):
        src = sbuf.at[i, pl.ds(b * RB, RB), :]
        dst = rbuf.at[1 + core, i // 2, pl.ds(b * RB, RB), :]
        return pltpu.make_async_remote_copy(
            src_ref=src, dst_ref=dst, send_sem=ss_sem.at[i, b], recv_sem=rr_sem.at[core, i // 2, b],
            device_id=dev(far + i % 2), device_id_type=MESH)

    def far_recv(s, c, b):
        ref = rbuf.at[1 + s, c, pl.ds(b * RB, RB), :]
        return pltpu.make_async_remote_copy(
            src_ref=ref, dst_ref=ref, send_sem=ss_sem.at[c, b], recv_sem=rr_sem.at[s, c, b],
            device_id=dev(partner), device_id_type=MESH)

    def part_send(c):
        return pltpu.make_async_remote_copy(
            src_ref=pbuf.at[c], dst_ref=rbuf.at[0, c], send_sem=sp_sem.at[c], recv_sem=rp_sem.at[c],
            device_id=dev(partner), device_id_type=MESH)

    a_copy.wait()
    pl.semaphore_wait(barrier, n_tp - 1)

    @pl.loop(0, half)
    def _(i):
        sbuf[i] = product(i).astype(jnp.bfloat16)
        far_send(i, 0).start()

    for b in range(1, nrb):
        @pl.loop(0, half)
        def _(i):
            far_send(i, b).start()

    @pl.loop(0, nch)
    def _(c):
        pbuf[c] = product(half + c).astype(jnp.bfloat16)
        part_send(c).start()

    r_copy.wait()
    g_copy.wait()

    @pl.loop(0, nch)
    def _(c):
        cols = pl.ds(pl.multiple_of(c * CN, CN), CN)
        own[c] = product(half + nch + c) + res[:, cols].astype(jnp.float32)

    @pl.loop(0, nch)
    def _(c):
        part_send(c).wait_recv()
        own[c] = own[c] + rbuf[0, c].astype(jnp.float32)

    def add_block(b, lo, hi):
        rs = pl.ds(b * RB, RB)

        @pl.loop(lo, hi)
        def _(c):
            cols = pl.ds(pl.multiple_of(c * CN, CN), CN)
            far_recv(0, c, b).wait_recv()
            far_recv(1, c, b).wait_recv()
            h = own[c, rs, :] + (rbuf[1, c, rs, :].astype(jnp.float32) + rbuf[2, c, rs, :].astype(jnp.float32))
            own[c, rs, :] = h
            hid_ref[rs, cols] = h.astype(jnp.bfloat16)
            h2 = h * h
            s = h2[:, :LANES]
            for k in range(1, CN // LANES):
                s = s + h2[:, k * LANES:(k + 1) * LANES]
            sq[b] = sq[b] + s

    def stat_copy(b, k):
        return pltpu.make_async_remote_copy(
            src_ref=st_out.at[b], dst_ref=st_in.at[b, k - 1], send_sem=sst_sem.at[b, k - 1],
            recv_sem=rst_sem.at[b, k - 1], device_id=dev((me + k) % n_tp), device_id_type=MESH)

    def send_stats(b):
        t = jnp.sum(sq[b].T, axis=0, keepdims=True)
        st_out[b] = jnp.broadcast_to(t, (8, RB))
        for k in range(1, n_tp):
            stat_copy(b, k).start()

    def normalise(b):
        rs = pl.ds(b * RB, RB)
        for k in range(1, n_tp):
            stat_copy(b, k).wait_recv()
        t = st_out[b] + st_in[b, 0] + st_in[b, 1] + st_in[b, 2]
        inv = lax.rsqrt(t / d_model + EPS)
        sq[b] = jnp.broadcast_to(inv[0:1], (LANES, RB)).T

        @pl.loop(0, nch)
        def _(c):
            for k in range(CN // LANES):
                cols = pl.ds(pl.multiple_of(c * CN + k * LANES, LANES), LANES)
                v = own[c, rs, k * LANES:(k + 1) * LANES] * sq[b] * gain[:, cols]
                nrm_ref[rs, cols] = v.astype(jnp.bfloat16)

    sq[...] = jnp.zeros_like(sq)
    for b in range(nrb):
        if b == 0:
            add_block(b, 0, nch)
        else:
            add_block(b, 0, nch // 2)
            normalise(b - 1)
            add_block(b, nch // 2, nch)
        send_stats(b)
    normalise(nrb - 1)

    @pl.loop(0, half)
    def _(i):
        for b in range(nrb):
            far_send(i, b).wait_send()

    @pl.loop(0, nch)
    def _(c):
        part_send(c).wait_send()

    for b in range(nrb):
        for k in range(1, n_tp):
            stat_copy(b, k).wait_send()


def solution(mesh):
    n_tp = mesh.shape["tp"]

    def local_step(attn_blk, w_blk, resid_blk, gain_blk):
        rows, depth = attn_blk.shape
        d_local = resid_blk.shape[1]
        nch = d_local // CN
        nrb = rows // RB
        out = jax.ShapeDtypeStruct((rows, d_local), jnp.bfloat16)
        bf, f32 = jnp.bfloat16, jnp.float32
        dma = pltpu.SemaphoreType.DMA
        return pl.pallas_call(
            functools.partial(kernel, n_tp),
            out_shape=(out, out),
            in_specs=[pl.BlockSpec(memory_space=pl.ANY)] * 4,
            out_specs=(pl.BlockSpec(memory_space=pltpu.VMEM),) * 2,
            scratch_shapes=[
                pltpu.VMEM((rows, depth), bf),
                pltpu.VMEM((4 * nch, depth, CN), bf),
                pltpu.VMEM((rows, d_local), bf),
                pltpu.VMEM((1, d_local), f32),
                pltpu.VMEM((2 * nch, rows, CN), bf),
                pltpu.VMEM((nch, rows, CN), bf),
                pltpu.VMEM((nch, rows, CN), f32),
                pltpu.VMEM((3, nch, rows, CN), bf),
                pltpu.VMEM((nrb, RB, LANES), f32),
                pltpu.VMEM((nrb, 8, RB), f32),
                pltpu.VMEM((nrb, n_tp - 1, 8, RB), f32),
                dma, dma((4 * nch,)), dma, dma,
                dma((2 * nch, nrb)), dma((nch,)),
                dma((2, nch, nrb)), dma((nch,)),
                dma((nrb, n_tp - 1)), dma((nrb, n_tp - 1)),
            ],
            compiler_params=pltpu.CompilerParams(
                collective_id=0, has_side_effects=True, vmem_limit_bytes=56 * 1024 * 1024),
        )(attn_blk, w_blk, resid_blk, gain_blk.reshape(1, d_local))

    return jax.shard_map(
        local_step,
        mesh=mesh,
        in_specs=(P("data", "tp"), P("tp", None), P("data", "tp"), P("tp")),
        out_specs=(P("data", "tp"), P("data", "tp")),
        check_vma=False,
    )
```

```python
import functools

import jax
import jax.numpy as jnp
from jax import lax
from jax.experimental import pallas as pl
from jax.experimental.pallas import tpu as pltpu
from jax.sharding import PartitionSpec as P

EPS = 1e-5
CN = 256
RB = 128
DEPTH = 6
LANES = 128
MESH = pl.DeviceIdType.MESH


def kernel(n_tp, a_hbm, w_hbm, r_hbm, g_hbm, hid_ref, nrm_ref,
           a, w, res, gain, sbuf, pbuf, own, rbuf, sq, st_out, st_in,
           a_sem, w_sem, r_sem, g_sem, ss_sem, sp_sem, rr_sem, rp_sem, sst_sem, rst_sem):
    rows, d_local = hid_ref.shape
    d_model = d_local * n_tp
    nch = d_local // CN
    nrb = rows // RB
    half = 2 * nch
    total = 4 * nch

    me = lax.axis_index("tp")
    chip = me // 2
    core = me % 2
    partner = chip * 2 + (1 - core)
    far = (1 - chip) * 2

    def dev(t):
        return {"tp": t}

    def owner_chunk(i):
        if isinstance(i, int):
            if i < half:
                return far + i % 2, i // 2
            if i < half + nch:
                return partner, i - half
            return me, i - half - nch
        is_far = jnp.int32(i < half)
        is_part = jnp.int32(i < half + nch) - is_far
        is_own = 1 - is_far - is_part
        o = is_far * (far + i % 2) + is_part * partner + is_own * me
        c = is_far * (i // 2) + is_part * (i - half) + is_own * (i - half - nch)
        return o, c

    def w_copy(i):
        o, c = owner_chunk(i)
        col = pl.multiple_of(o * d_local + c * CN, CN)
        return pltpu.make_async_copy(w_hbm.at[:, pl.ds(col, CN)], w.at[i], w_sem.at[i])

    a_copy = pltpu.make_async_copy(a_hbm, a, a_sem)
    a_copy.start()
    for i in range(DEPTH):
        w_copy(i).start()
    r_copy = pltpu.make_async_copy(r_hbm, res, r_sem)
    r_copy.start()
    g_copy = pltpu.make_async_copy(g_hbm, gain, g_sem)
    g_copy.start()

    barrier = pltpu.get_barrier_semaphore()
    for k in range(1, n_tp):
        pl.semaphore_signal(barrier, inc=1, device_id=dev((me + k) % n_tp), device_id_type=MESH)

    def product(i):
        @pl.when(i + DEPTH < total)
        def _():
            w_copy(i + DEPTH).start()

        w_copy(i).wait()
        return jnp.dot(a[...], w[i], preferred_element_type=jnp.float32)

    def far_send(i, b):
        src = sbuf.at[i, pl.ds(b * RB, RB), :]
        dst = rbuf.at[1 + core, i // 2, pl.ds(b * RB, RB), :]
        return pltpu.make_async_remote_copy(
            src_ref=src, dst_ref=dst, send_sem=ss_sem.at[i, b], recv_sem=rr_sem.at[core, i // 2, b],
            device_id=dev(far + i % 2), device_id_type=MESH)

    def far_recv(s, c, b):
        ref = rbuf.at[1 + s, c, pl.ds(b * RB, RB), :]
        return pltpu.make_async_remote_copy(
            src_ref=ref, dst_ref=ref, send_sem=ss_sem.at[c, b], recv_sem=rr_sem.at[s, c, b],
            device_id=dev(partner), device_id_type=MESH)

    def part_send(c):
        return pltpu.make_async_remote_copy(
            src_ref=pbuf.at[c], dst_ref=rbuf.at[0, c], send_sem=sp_sem.at[c], recv_sem=rp_sem.at[c],
            device_id=dev(partner), device_id_type=MESH)

    with jax.named_scope("a_wait"):
        a_copy.wait()
    with jax.named_scope("barrier_wait"):
        pl.semaphore_wait(barrier, n_tp - 1)

    @pl.loop(0, half)
    def _(i):
        with jax.named_scope("far_product"):
            sbuf[i] = product(i).astype(jnp.bfloat16)
        far_send(i, 0).start()

    for b in range(1, nrb):
        @pl.loop(0, half)
        def _(i):
            far_send(i, b).start()

    @pl.loop(0, nch)
    def _(c):
        with jax.named_scope("part_product"):
            pbuf[c] = product(half + c).astype(jnp.bfloat16)
        part_send(c).start()

    r_copy.wait()
    g_copy.wait()

    @pl.loop(0, nch)
    def _(c):
        cols = pl.ds(pl.multiple_of(c * CN, CN), CN)
        with jax.named_scope("own_product"):
            own[c] = product(half + nch + c) + res[:, cols].astype(jnp.float32)

    @pl.loop(0, nch)
    def _(c):
        part_send(c).wait_recv()
        own[c] = own[c] + rbuf[0, c].astype(jnp.float32)

    def add_block(b, lo, hi):
        rs = pl.ds(b * RB, RB)

        @pl.loop(lo, hi)
        def _(c):
            cols = pl.ds(pl.multiple_of(c * CN, CN), CN)
            with jax.named_scope(f"far_wait{b}"):
                far_recv(0, c, b).wait_recv()
                far_recv(1, c, b).wait_recv()
            h = own[c, rs, :] + (rbuf[1, c, rs, :].astype(jnp.float32) + rbuf[2, c, rs, :].astype(jnp.float32))
            own[c, rs, :] = h
            hid_ref[rs, cols] = h.astype(jnp.bfloat16)
            h2 = h * h
            s = h2[:, :LANES]
            for k in range(1, CN // LANES):
                s = s + h2[:, k * LANES:(k + 1) * LANES]
            sq[b] = sq[b] + s

    def stat_copy(b, k):
        return pltpu.make_async_remote_copy(
            src_ref=st_out.at[b], dst_ref=st_in.at[b, k - 1], send_sem=sst_sem.at[b, k - 1],
            recv_sem=rst_sem.at[b, k - 1], device_id=dev((me + k) % n_tp), device_id_type=MESH)

    def send_stats(b):
        with jax.named_scope(f"send_stats{b}"):
            t = jnp.sum(sq[b].T, axis=0, keepdims=True)
            st_out[b] = jnp.broadcast_to(t, (8, RB))
            for k in range(1, n_tp):
                stat_copy(b, k).start()

    def normalise(b):
        rs = pl.ds(b * RB, RB)
        with jax.named_scope(f"stat_wait{b}"):
            for k in range(1, n_tp):
                stat_copy(b, k).wait_recv()
        t = st_out[b] + st_in[b, 0] + st_in[b, 1] + st_in[b, 2]
        inv = lax.rsqrt(t / d_model + EPS)
        sq[b] = jnp.broadcast_to(inv[0:1], (LANES, RB)).T

        @pl.loop(0, nch)
        def _(c):
            for k in range(CN // LANES):
                cols = pl.ds(pl.multiple_of(c * CN + k * LANES, LANES), LANES)
                v = own[c, rs, k * LANES:(k + 1) * LANES] * sq[b] * gain[:, cols]
                nrm_ref[rs, cols] = v.astype(jnp.bfloat16)

    sq[...] = jnp.zeros_like(sq)
    for b in range(nrb):
        if b == 0:
            add_block(b, 0, nch)
        else:
            add_block(b, 0, nch // 2)
            normalise(b - 1)
            add_block(b, nch // 2, nch)
        send_stats(b)
    normalise(nrb - 1)

    with jax.named_scope("drain"):
        @pl.loop(0, half)
        def _(i):
            for b in range(nrb):
                far_send(i, b).wait_send()

    @pl.loop(0, nch)
    def _(c):
        part_send(c).wait_send()

    for b in range(nrb):
        for k in range(1, n_tp):
            stat_copy(b, k).wait_send()


def solution(mesh):
    n_tp = mesh.shape["tp"]

    def local_step(attn_blk, w_blk, resid_blk, gain_blk):
        rows, depth = attn_blk.shape
        d_local = resid_blk.shape[1]
        nch = d_local // CN
        nrb = rows // RB
        out = pltpu.VMEM((rows, d_local), jnp.bfloat16)
        bf, f32 = jnp.bfloat16, jnp.float32
        dma = pltpu.SemaphoreType.DMA
        return pl.pallas_call(
            functools.partial(kernel, n_tp),
            out_shape=(out, out),
            in_specs=[pl.BlockSpec(memory_space=pl.ANY)] * 4,
            out_specs=(pl.BlockSpec(memory_space=pltpu.VMEM),) * 2,
            scratch_shapes=[
                pltpu.VMEM((rows, depth), bf),
                pltpu.VMEM((4 * nch, depth, CN), bf),
                pltpu.VMEM((rows, d_local), bf),
                pltpu.VMEM((1, d_local), f32),
                pltpu.VMEM((2 * nch, rows, CN), bf),
                pltpu.VMEM((nch, rows, CN), bf),
                pltpu.VMEM((nch, rows, CN), f32),
                pltpu.VMEM((3, nch, rows, CN), bf),
                pltpu.VMEM((nrb, RB, LANES), f32),
                pltpu.VMEM((nrb, 8, RB), f32),
                pltpu.VMEM((nrb, n_tp - 1, 8, RB), f32),
                dma, dma((4 * nch,)), dma, dma,
                dma((2 * nch, nrb)), dma((nch,)),
                dma((2, nch, nrb)), dma((nch,)),
                dma((nrb, n_tp - 1)), dma((nrb, n_tp - 1)),
            ],
            compiler_params=pltpu.CompilerParams(
                collective_id=0, has_side_effects=True, vmem_limit_bytes=56 * 1024 * 1024),
        )(attn_blk, w_blk, resid_blk, gain_blk.reshape(1, d_local))

    return jax.shard_map(
        local_step,
        mesh=mesh,
        in_specs=(P("data", "tp"), P("tp", None), P("data", "tp"), P("tp")),
        out_specs=(P("data", "tp"), P("data", "tp")),
        check_vma=False,
    )
```

```python
import functools

import jax
import jax.numpy as jnp
from jax import lax
from jax.experimental import pallas as pl
from jax.experimental.pallas import tpu as pltpu
from jax.sharding import PartitionSpec as P

EPS = 1e-5
CN = 256
RB = 128
DEPTH = 6
WSEM = 8
LEAD = 3
LANES = 128
MESH = pl.DeviceIdType.MESH


def fold(x):
    s = x[:, :LANES]
    for k in range(1, x.shape[1] // LANES):
        s = s + x[:, k * LANES:(k + 1) * LANES]
    return s


def main_kernel(n_tp, a_hbm, w_hbm, r_hbm, g_hbm,
                hid_ref, nrm_ref, last_ref, scale_ref, gain,
                a, w, res, sbuf, pbuf, own, rbuf, sq, st_out, st_in,
                a_sem, w_sem, r_sem, g_sem, ss_sem, sp_sem, rr_sem, rp_sem, sst_sem, rst_sem):
    rows, d_local = hid_ref.shape
    d_model = d_local * n_tp
    nch = d_local // CN
    nrb = rows // RB
    half = 2 * nch
    total = 4 * nch
    last = nrb - 1

    me = lax.axis_index("tp")
    chip = me // 2
    core = me % 2
    partner = chip * 2 + (1 - core)
    far = (1 - chip) * 2

    def dev(t):
        return {"tp": t}

    def block(b):
        return pl.ds(b * RB, RB)

    def w_copy(i):
        if isinstance(i, int):
            i = jnp.int32(i)
        is_far = jnp.int32(i < half)
        is_part = jnp.int32(i < half + nch) - is_far
        is_own = 1 - is_far - is_part
        o = is_far * (far + i % 2) + is_part * partner + is_own * me
        c = is_far * (i // 2) + is_part * (i - half) + is_own * (i - half - nch)
        col = pl.multiple_of(o * d_local + c * CN, CN)
        return pltpu.make_async_copy(w_hbm.at[:, pl.ds(col, CN)], w.at[i], w_sem.at[i % WSEM])

    def a_copy(k):
        rs = pl.ds(k * (rows // 2), rows // 2)
        return pltpu.make_async_copy(a_hbm.at[rs], a.at[rs], a_sem.at[k])

    a_copy(0).start()
    w_copy(0).start()
    barrier = pltpu.get_barrier_semaphore()
    for k in range(1, n_tp):
        pl.semaphore_signal(barrier, inc=1, device_id=dev((me + k) % n_tp), device_id_type=MESH)
    with jax.named_scope("barrier_wait"):
        pl.semaphore_wait(barrier, n_tp - 1)
    a_copy(1).start()
    for i in range(1, DEPTH):
        w_copy(i).start()
    r_copy = pltpu.make_async_copy(r_hbm, res, r_sem)
    g_copy = pltpu.make_async_copy(g_hbm, gain, g_sem)
    r_copy.start()
    g_copy.start()

    def product(i):
        @pl.when(i + DEPTH < total)
        def _():
            w_copy(i + DEPTH).start()

        w_copy(i).wait()
        return jnp.dot(a[...], w[i], preferred_element_type=jnp.float32)

    def far_send(i, b):
        return pltpu.make_async_remote_copy(
            src_ref=sbuf.at[i, block(b), :], dst_ref=rbuf.at[1 + core, i // 2, block(b), :],
            send_sem=ss_sem, recv_sem=rr_sem.at[i // 2, b],
            device_id=dev(far + i % 2), device_id_type=MESH)

    def local_wait(ref, sem):
        pltpu.make_async_copy(ref, ref, sem).wait()

    def part_send(c):
        return pltpu.make_async_remote_copy(
            src_ref=pbuf.at[c], dst_ref=rbuf.at[0, c], send_sem=sp_sem, recv_sem=rp_sem,
            device_id=dev(partner), device_id_type=MESH)

    with jax.named_scope("a_wait"):
        a_copy(0).wait()
    with jax.named_scope("w0_wait"):
        w_copy(0).wait()
    hr = rows // 2
    with jax.named_scope("first"):
        sbuf[0, :hr] = jnp.dot(a[:hr], w[0], preferred_element_type=jnp.float32).astype(jnp.bfloat16)
    far_send(0, 0).start()
    w_copy(DEPTH).start()
    a_copy(1).wait()

    @pl.loop(1, half)
    def _(i):
        with jax.named_scope("far_product"):
            sbuf[i] = product(i).astype(jnp.bfloat16)
        far_send(i, 0).start()

    sbuf[0, hr:] = jnp.dot(a[hr:], w[0], preferred_element_type=jnp.float32).astype(jnp.bfloat16)

    @pl.loop(0, nch)
    def _(c):
        with jax.named_scope("part_product"):
            pbuf[c] = product(half + c).astype(jnp.bfloat16)
        part_send(c).start()

    r_copy.wait()
    g_copy.wait()

    @pl.loop(0, nch)
    def _(c):
        cols = pl.ds(pl.multiple_of(c * CN, CN), CN)
        with jax.named_scope("own_product"):
            own[c] = product(half + nch + c) + res[:, cols].astype(jnp.float32)

    local_wait(rbuf.at[0], rp_sem)

    @pl.loop(0, nch)
    def _(c):
        own[c] = own[c] + rbuf[0, c].astype(jnp.float32)

    def issue(q):
        b, c = divmod(q, nch)
        if 1 <= b < nrb:
            far_send(2 * c, b).start()
            far_send(2 * c + 1, b).start()

    def add_chunk(b, c):
        cols = pl.ds(c * CN, CN)
        with jax.named_scope(f"far_wait{b}"):
            local_wait(rbuf.at[pl.ds(1, 2), c, block(b), :], rr_sem.at[c, b])
        issue(b * nch + c + LEAD)
        rs = block(b)
        h = own[c, rs, :] + (rbuf[1, c, rs, :].astype(jnp.float32) + rbuf[2, c, rs, :].astype(jnp.float32))
        hid_ref[rs, cols] = h.astype(jnp.bfloat16)
        if b == last:
            last_ref[:, cols] = h
        else:
            own[c, rs, :] = h
        s = fold(h * h)
        sq[b] = s if c == 0 else sq[b] + s

    def stat_copy(b, k):
        return pltpu.make_async_remote_copy(
            src_ref=st_out.at[b], dst_ref=st_in.at[b, k - 1], send_sem=sst_sem.at[b],
            recv_sem=rst_sem.at[b], device_id=dev((me + k) % n_tp), device_id_type=MESH)

    def send_stats(b):
        with jax.named_scope(f"send_stats{b}"):
            t = jnp.sum(sq[b].T, axis=0, keepdims=True)
            st_out[b] = jnp.broadcast_to(t, (8, RB))
            for k in range(1, n_tp):
                stat_copy(b, k).start()

    def scale(b):
        with jax.named_scope(f"stat_wait{b}"):
            local_wait(st_in.at[b], rst_sem.at[b])
        t = st_out[b] + st_in[b, 0] + st_in[b, 1] + st_in[b, 2]
        inv = lax.rsqrt(t / d_model + EPS)
        return jnp.broadcast_to(inv[0:1], (LANES, RB)).T

    def normalise(b):
        sq[b] = scale(b)

        @pl.loop(0, nch)
        def _(c):
            for k in range(CN // LANES):
                cols = pl.ds(pl.multiple_of(c * CN + k * LANES, LANES), LANES)
                v = own[c, block(b), k * LANES:(k + 1) * LANES] * sq[b] * gain[:, cols]
                nrm_ref[block(b), cols] = v.astype(jnp.bfloat16)

    for b in range(nrb):
        for c in range(nch):
            if b > 0 and c == LEAD + 2:
                normalise(b - 1)
            add_chunk(b, c)
        send_stats(b)

    with jax.named_scope("drain"):
        local_wait(sbuf, ss_sem)
        local_wait(pbuf, sp_sem)
        for b in range(last):
            local_wait(st_in.at[b], sst_sem.at[b])
    scale_ref[...] = scale(last)
    with jax.named_scope("drain2"):
        local_wait(st_in.at[last], sst_sem.at[last])


def finish_kernel(hid_ref, nrm_ref, last_ref, scale_ref, gain_ref, hid_hbm, nrm_hbm, buf, sem):
    rows, d_local = hid_hbm.shape
    early = nrm_ref.shape[0]
    late = pl.ds(early, rows - early)
    copies = [
        pltpu.make_async_copy(hid_ref, hid_hbm, sem.at[0]),
        pltpu.make_async_copy(nrm_ref, nrm_hbm.at[pl.ds(0, early)], sem.at[1]),
    ]
    for c in copies:
        c.start()

    @pl.loop(0, d_local // LANES)
    def _(j):
        cols = pl.ds(pl.multiple_of(j * LANES, LANES), LANES)
        buf[:, cols] = (last_ref[:, cols] * scale_ref[...] * gain_ref[:, cols]).astype(jnp.bfloat16)

    copies.append(pltpu.make_async_copy(buf, nrm_hbm.at[late], sem.at[2]))
    copies[-1].start()
    for c in copies:
        c.wait()


def solution(mesh):
    n_tp = mesh.shape["tp"]

    def local_step(attn_blk, w_blk, resid_blk, gain_blk):
        rows, depth = attn_blk.shape
        d_local = resid_blk.shape[1]
        nch = d_local // CN
        nrb = rows // RB
        bf, f32 = jnp.bfloat16, jnp.float32
        dma = pltpu.SemaphoreType.DMA
        vmem = pl.BlockSpec(memory_space=pltpu.VMEM)
        hbm = pl.BlockSpec(memory_space=pl.ANY)
        parts = pl.pallas_call(
            functools.partial(main_kernel, n_tp),
            out_shape=(
                pltpu.VMEM((rows, d_local), bf),
                pltpu.VMEM((rows - RB, d_local), bf),
                pltpu.VMEM((RB, d_local), f32),
                pltpu.VMEM((RB, LANES), f32),
                pltpu.VMEM((1, d_local), f32),
            ),
            in_specs=[hbm] * 4,
            out_specs=(vmem,) * 5,
            scratch_shapes=[
                pltpu.VMEM((rows, depth), bf),
                pltpu.VMEM((4 * nch, depth, CN), bf),
                pltpu.VMEM((rows, d_local), bf),
                pltpu.VMEM((2 * nch, rows, CN), bf),
                pltpu.VMEM((nch, rows, CN), bf),
                pltpu.VMEM((nch, rows, CN), f32),
                pltpu.VMEM((3, nch, rows, CN), bf),
                pltpu.VMEM((nrb, RB, LANES), f32),
                pltpu.VMEM((nrb, 8, RB), f32),
                pltpu.VMEM((nrb, n_tp - 1, 8, RB), f32),
                dma((2,)), dma((WSEM,)), dma, dma,
                dma, dma, dma((nch, nrb)), dma, dma((nrb,)), dma((nrb,)),
            ],
            compiler_params=pltpu.CompilerParams(
                collective_id=0, has_side_effects=True, vmem_limit_bytes=54 * 1024 * 1024),
        )(attn_blk, w_blk, resid_blk, gain_blk.reshape(1, d_local))
        out = jax.ShapeDtypeStruct((rows, d_local), bf)
        return pl.pallas_call(
            finish_kernel,
            out_shape=(out, out),
            in_specs=[vmem] * 5,
            out_specs=(hbm, hbm),
            scratch_shapes=[pltpu.VMEM((RB, d_local), bf), dma((3,))],
            compiler_params=pltpu.CompilerParams(vmem_limit_bytes=4 * 1024 * 1024),
        )(*parts)

    return jax.shard_map(
        local_step,
        mesh=mesh,
        in_specs=(P("data", "tp"), P("tp", None), P("data", "tp"), P("tp")),
        out_specs=(P("data", "tp"), P("data", "tp")),
        check_vma=False,
    )
```

```python
import functools

import jax
import jax.numpy as jnp
from jax import lax
from jax.experimental import pallas as pl
from jax.experimental.pallas import tpu as pltpu
from jax.sharding import PartitionSpec as P

EPS = 1e-5
CN = 256
RB = 128
DEPTH = 6
WSEM = 8
LEAD = 3
LANES = 128
MESH = pl.DeviceIdType.MESH


def fold(x):
    s = x[:, :LANES]
    for k in range(1, x.shape[1] // LANES):
        s = s + x[:, k * LANES:(k + 1) * LANES]
    return s


def spread(inv):
    return jnp.broadcast_to(inv[0:1], (LANES, inv.shape[1])).T


def main_kernel(n_tp, a_hbm, w_hbm, r_hbm, g_hbm,
                hid_ref, nrm_ref, last_ref, scale_ref, gain,
                a, w, res, sbuf, pbuf, own, rbuf, sq, st_out, st_in,
                a_sem, w0_sem, w_sem, r_sem, g_sem, ss_sem, sp_sem, rr_sem, rp_sem, sst_sem, rst_sem):
    rows, d_local = hid_ref.shape
    d_model = d_local * n_tp
    nch = d_local // CN
    nrb = rows // RB
    half = 2 * nch
    total = 4 * nch
    last = nrb - 1

    me = lax.axis_index("tp")
    chip = me // 2
    core = me % 2
    partner = chip * 2 + (1 - core)
    far = (1 - chip) * 2

    def dev(t):
        return {"tp": t}

    def block(b):
        return pl.ds(b * RB, RB)

    def w_copy(i):
        if isinstance(i, int):
            i = jnp.int32(i)
        is_far = jnp.int32(i < half)
        is_part = jnp.int32(i < half + nch) - is_far
        is_own = 1 - is_far - is_part
        o = is_far * (far + i % 2) + is_part * partner + is_own * me
        c = is_far * (i // 2) + is_part * (i - half) + is_own * (i - half - nch)
        col = pl.multiple_of(o * d_local + c * CN, CN)
        return pltpu.make_async_copy(w_hbm.at[:, pl.ds(col, CN)], w.at[i], w_sem.at[i % WSEM])

    def a_copy(k):
        rs = pl.ds(k * (rows // 2), rows // 2)
        return pltpu.make_async_copy(a_hbm.at[rs], a.at[rs], a_sem.at[k])

    def w_piece(p):
        col = pl.multiple_of(far * d_local + p * LANES, LANES)
        return pltpu.make_async_copy(
            w_hbm.at[:, pl.ds(col, LANES)], w.at[0, :, pl.ds(p * LANES, LANES)], w0_sem.at[p])

    barrier = pltpu.get_barrier_semaphore()
    for k in range(1, n_tp):
        pl.semaphore_signal(barrier, inc=1, device_id=dev((me + k) % n_tp), device_id_type=MESH)
    a_copy(0).start()
    for p in range(CN // LANES):
        w_piece(p).start()
    r_copy = pltpu.make_async_copy(r_hbm, res, r_sem)
    g_copy = pltpu.make_async_copy(g_hbm, gain, g_sem)

    def product(i):
        @pl.when(i + DEPTH < total)
        def _():
            w_copy(i + DEPTH).start()

        w_copy(i).wait()
        return jnp.dot(a[...], w[i], preferred_element_type=jnp.float32)

    def far_send(i, b):
        return pltpu.make_async_remote_copy(
            src_ref=sbuf.at[i, block(b), :], dst_ref=rbuf.at[1 + core, i // 2, block(b), :],
            send_sem=ss_sem, recv_sem=rr_sem.at[i // 2, b],
            device_id=dev(far + i % 2), device_id_type=MESH)

    def local_wait(ref, sem):
        pltpu.make_async_copy(ref, ref, sem).wait()

    def part_send(c):
        return pltpu.make_async_remote_copy(
            src_ref=pbuf.at[c], dst_ref=rbuf.at[0, c], send_sem=sp_sem, recv_sem=rp_sem,
            device_id=dev(partner), device_id_type=MESH)

    with jax.named_scope("a_wait"):
        a_copy(0).wait()
    a_copy(1).start()
    w_copy(1).start()
    hr = rows // 2
    for p in range(CN // LANES):
        cols = pl.ds(p * LANES, LANES)
        with jax.named_scope(f"w0_wait{p}"):
            w_piece(p).wait()
        with jax.named_scope(f"first{p}"):
            sbuf[0, :hr, cols] = jnp.dot(
                a[:hr], w[0, :, cols], preferred_element_type=jnp.float32).astype(jnp.bfloat16)
        if p == 0:
            with jax.named_scope("barrier_wait"):
                pl.semaphore_wait(barrier, n_tp - 1)
        pltpu.make_async_remote_copy(
            src_ref=sbuf.at[0, block(0), cols], dst_ref=rbuf.at[1 + core, 0, block(0), cols],
            send_sem=ss_sem, recv_sem=rr_sem.at[0, 0], device_id=dev(far), device_id_type=MESH).start()
    for i in range(2, DEPTH + 1):
        w_copy(i).start()
    r_copy.start()
    g_copy.start()
    with jax.named_scope("a_wait1"):
        a_copy(1).wait()

    @pl.loop(1, half)
    def _(i):
        with jax.named_scope("far_product"):
            sbuf[i] = product(i).astype(jnp.bfloat16)
        far_send(i, 0).start()

    sbuf[0, hr:] = jnp.dot(a[hr:], w[0], preferred_element_type=jnp.float32).astype(jnp.bfloat16)

    @pl.loop(0, nch)
    def _(c):
        with jax.named_scope("part_product"):
            pbuf[c] = product(half + c).astype(jnp.bfloat16)
        part_send(c).start()

    r_copy.wait()
    g_copy.wait()

    @pl.loop(0, nch)
    def _(c):
        cols = pl.ds(pl.multiple_of(c * CN, CN), CN)
        with jax.named_scope("own_product"):
            own[c] = product(half + nch + c) + res[:, cols].astype(jnp.float32)

    local_wait(rbuf.at[0], rp_sem)

    @pl.loop(0, nch)
    def _(c):
        own[c] = own[c] + rbuf[0, c].astype(jnp.float32)

    def issue(q):
        b, c = divmod(q, nch)
        if 1 <= b < nrb:
            far_send(2 * c, b).start()
            far_send(2 * c + 1, b).start()

    def add_chunk(b, c):
        cols = pl.ds(c * CN, CN)
        with jax.named_scope(f"far_wait{b}"):
            local_wait(rbuf.at[pl.ds(1, 2), c, block(b), :], rr_sem.at[c, b])
        issue(b * nch + c + LEAD)
        rs = block(b)
        h = own[c, rs, :] + (rbuf[1, c, rs, :].astype(jnp.float32) + rbuf[2, c, rs, :].astype(jnp.float32))
        hid_ref[rs, cols] = h.astype(jnp.bfloat16)
        if b == last:
            last_ref[:, cols] = h
        else:
            own[c, rs, :] = h
        s = fold(h * h)
        sq[b] = s if c == 0 else sq[b] + s

    def stat_copy(b, k):
        return pltpu.make_async_remote_copy(
            src_ref=st_out.at[b], dst_ref=st_in.at[b, k - 1], send_sem=sst_sem.at[b],
            recv_sem=rst_sem.at[b], device_id=dev((me + k) % n_tp), device_id_type=MESH)

    def send_stats(b):
        with jax.named_scope(f"send_stats{b}"):
            t = jnp.sum(sq[b].T, axis=0, keepdims=True)
            st_out[b] = jnp.broadcast_to(t, (8, RB))
            for k in range(1, n_tp):
                stat_copy(b, k).start()

    def scale(b):
        with jax.named_scope(f"stat_wait{b}"):
            local_wait(st_in.at[b], rst_sem.at[b])
        t = st_out[b] + st_in[b, 0] + st_in[b, 1] + st_in[b, 2]
        return lax.rsqrt(t / d_model + EPS)

    def normalise(b):
        sq[b] = spread(scale(b))

        @pl.loop(0, nch)
        def _(c):
            for k in range(CN // LANES):
                cols = pl.ds(pl.multiple_of(c * CN + k * LANES, LANES), LANES)
                v = own[c, block(b), k * LANES:(k + 1) * LANES] * sq[b] * gain[:, cols]
                nrm_ref[block(b), cols] = v.astype(jnp.bfloat16)

    for b in range(nrb):
        for c in range(nch):
            if b > 0 and c == LEAD + 2:
                normalise(b - 1)
            add_chunk(b, c)
        send_stats(b)

    with jax.named_scope("drain"):
        local_wait(sbuf, ss_sem)
        local_wait(pbuf, sp_sem)
        for b in range(last):
            local_wait(st_in.at[b], sst_sem.at[b])
    scale_ref[...] = scale(last)
    with jax.named_scope("drain2"):
        local_wait(st_in.at[last], sst_sem.at[last])


def finish_kernel(hid_ref, nrm_ref, last_ref, scale_ref, gain_ref, hid_hbm, nrm_hbm, buf, scale, sem):
    rows, d_local = hid_hbm.shape
    early = nrm_ref.shape[0]
    late = pl.ds(early, rows - early)
    copies = [
        pltpu.make_async_copy(hid_ref, hid_hbm, sem.at[0]),
        pltpu.make_async_copy(nrm_ref, nrm_hbm.at[pl.ds(0, early)], sem.at[1]),
    ]
    for c in copies:
        c.start()

    scale[...] = spread(scale_ref[...])

    @pl.loop(0, d_local // LANES)
    def _(j):
        cols = pl.ds(pl.multiple_of(j * LANES, LANES), LANES)
        buf[:, cols] = (last_ref[:, cols] * scale[...] * gain_ref[:, cols]).astype(jnp.bfloat16)

    copies.append(pltpu.make_async_copy(buf, nrm_hbm.at[late], sem.at[2]))
    copies[-1].start()
    for c in copies:
        c.wait()


def solution(mesh):
    n_tp = mesh.shape["tp"]

    def local_step(attn_blk, w_blk, resid_blk, gain_blk):
        rows, depth = attn_blk.shape
        d_local = resid_blk.shape[1]
        nch = d_local // CN
        nrb = rows // RB
        bf, f32 = jnp.bfloat16, jnp.float32
        dma = pltpu.SemaphoreType.DMA
        vmem = pl.BlockSpec(memory_space=pltpu.VMEM)
        hbm = pl.BlockSpec(memory_space=pl.ANY)
        parts = pl.pallas_call(
            functools.partial(main_kernel, n_tp),
            out_shape=(
                pltpu.VMEM((rows, d_local), bf),
                pltpu.VMEM((rows - RB, d_local), bf),
                pltpu.VMEM((RB, d_local), f32),
                pltpu.VMEM((8, RB), f32),
                pltpu.VMEM((1, d_local), f32),
            ),
            in_specs=[hbm] * 4,
            out_specs=(vmem,) * 5,
            scratch_shapes=[
                pltpu.VMEM((rows, depth), bf),
                pltpu.VMEM((4 * nch, depth, CN), bf),
                pltpu.VMEM((rows, d_local), bf),
                pltpu.VMEM((2 * nch, rows, CN), bf),
                pltpu.VMEM((nch, rows, CN), bf),
                pltpu.VMEM((nch, rows, CN), f32),
                pltpu.VMEM((3, nch, rows, CN), bf),
                pltpu.VMEM((nrb, RB, LANES), f32),
                pltpu.VMEM((nrb, 8, RB), f32),
                pltpu.VMEM((nrb, n_tp - 1, 8, RB), f32),
                dma((2,)), dma((CN // LANES,)), dma((WSEM,)), dma, dma,
                dma, dma, dma((nch, nrb)), dma, dma((nrb,)), dma((nrb,)),
            ],
            compiler_params=pltpu.CompilerParams(
                collective_id=0, has_side_effects=True, vmem_limit_bytes=54 * 1024 * 1024),
        )(attn_blk, w_blk, resid_blk, gain_blk.reshape(1, d_local))
        out = jax.ShapeDtypeStruct((rows, d_local), bf)
        return pl.pallas_call(
            finish_kernel,
            out_shape=(out, out),
            in_specs=[vmem] * 5,
            out_specs=(hbm, hbm),
            scratch_shapes=[pltpu.VMEM((RB, d_local), bf), pltpu.VMEM((RB, LANES), f32), dma((3,))],
            compiler_params=pltpu.CompilerParams(vmem_limit_bytes=4 * 1024 * 1024),
        )(*parts)

    return jax.shard_map(
        local_step,
        mesh=mesh,
        in_specs=(P("data", "tp"), P("tp", None), P("data", "tp"), P("tp")),
        out_specs=(P("data", "tp"), P("data", "tp")),
        check_vma=False,
    )
```

```python
import functools

import jax
import jax.numpy as jnp
from jax import lax
from jax.experimental import pallas as pl
from jax.experimental.pallas import tpu as pltpu
from jax.sharding import PartitionSpec as P

EPS = 1e-5
CN = 256
RB = 128
DEPTH = 4
WSEM = 4
LANES = 128
MESH = pl.DeviceIdType.MESH


def fold(x):
    s = x[:, :LANES]
    for k in range(1, x.shape[1] // LANES):
        s = s + x[:, k * LANES:(k + 1) * LANES]
    return s


def spread(inv):
    return jnp.broadcast_to(inv[0:1], (LANES, inv.shape[1])).T


def main_kernel(n_tp, a_hbm, w_hbm, r_hbm, g_hbm,
                hid_ref, nrm_ref, last_ref, scale_ref, gain,
                a, w, res, sbuf, own, rbuf, sq, st_out, st_in,
                head_sem, late_sem, w_sem, send_sem, far_sem, part_sem, sst_sem, rst_sem):
    rows, d_local = hid_ref.shape
    d_model = d_local * n_tp
    nch = d_local // CN
    nrb = rows // RB
    half = 2 * nch
    last = nrb - 1
    bf, f32 = jnp.bfloat16, jnp.float32

    me = lax.axis_index("tp")
    chip = me // 2
    core = me % 2
    partner = chip * 2 + (1 - core)
    far = (1 - chip) * 2

    def dev(t):
        return {"tp": t}

    def block(b):
        return pl.ds(b * RB, RB)

    def wait(ref, sem):
        pltpu.make_async_copy(ref, ref, sem).wait()

    def w_pair(j, act):
        is_far = jnp.int32(j < nch)
        k = j - nch
        is_part = jnp.int32(k < nch // 2) * (1 - is_far)
        is_own = 1 - is_far - is_part
        near = is_part * partner + is_own * me
        base = is_far * (far * nch + j) + (1 - is_far) * (near * nch + 2 * (k - is_own * (nch // 2)))
        step = is_far * nch + (1 - is_far)
        for p in range(2):
            col = pl.multiple_of((base + p * step) * CN, CN)
            act(pltpu.make_async_copy(w_hbm.at[:, pl.ds(col, CN)], w.at[2 * j + p], w_sem.at[j % WSEM]))

    def w_start(j):
        w_pair(j, lambda c: c.start())

    def w_wait(j):
        wait(w.at[pl.ds(2 * j, 2)], w_sem.at[j % WSEM])

    hc = CN // 2

    def w_piece(p):
        col = pl.multiple_of(far * d_local + p * hc, hc)
        return pltpu.make_async_copy(w_hbm.at[:, pl.ds(col, hc)], w.at[0, :, pl.ds(p * hc, hc)], head_sem.at[1 + p])

    def w_second():
        col = pl.multiple_of((far + 1) * d_local, CN)
        return pltpu.make_async_copy(w_hbm.at[:, pl.ds(col, CN)], w.at[1], w_sem.at[0])

    def far_send(i, b):
        return pltpu.make_async_remote_copy(
            src_ref=sbuf.at[i, block(b), :], dst_ref=rbuf.at[1 + core, i // 2, block(b), :],
            send_sem=send_sem, recv_sem=far_sem.at[group_of(i // 2, b)],
            device_id=dev(far + i % 2), device_id_type=MESH)

    quarter = nch // 2

    def group_of(c, b):
        if b < last:
            return b * 2 + c // quarter
        g = last * 2
        if isinstance(c, int):
            return g + (0 if c < quarter else 1 if c < nch - 2 else c - (nch - 2) + 2)
        return g + jnp.int32(c >= quarter) + jnp.int32(c >= nch - 2) + jnp.int32(c >= nch - 1)

    def groups(b):
        if b < last:
            return [(0, quarter), (quarter, nch)]
        return [(0, quarter), (quarter, nch - 2), (nch - 2, nch - 1), (nch - 1, nch)]

    a_top, a_bot = (pltpu.make_async_copy(a_hbm.at[pl.ds(k * RB, RB * (1 if k == 0 else nrb - 1))],
                                          a.at[pl.ds(k * RB, RB * (1 if k == 0 else nrb - 1))],
                                          head_sem.at[0] if k == 0 else late_sem) for k in range(2))
    r_copy = pltpu.make_async_copy(r_hbm, res, late_sem)
    g_copy = pltpu.make_async_copy(g_hbm, gain, late_sem)

    barrier = pltpu.get_barrier_semaphore()
    for k in range(1, n_tp):
        pl.semaphore_signal(barrier, inc=1, device_id=dev((me + k) % n_tp), device_id_type=MESH)
    a_top.start()
    w_piece(0).start()
    w_piece(1).start()

    def top_product(i):
        sbuf[i, :RB] = jnp.dot(a[:RB], w[i], preferred_element_type=f32).astype(bf)

    with jax.named_scope("a_wait"):
        a_top.wait()
    w_second().start()

    def piece_send(p):
        cols = pl.ds(p * hc, hc)
        pltpu.make_async_remote_copy(
            src_ref=sbuf.at[0, block(0), cols], dst_ref=rbuf.at[1 + core, 0, block(0), cols],
            send_sem=send_sem, recv_sem=far_sem.at[group_of(0, 0)], device_id=dev(far), device_id_type=MESH).start()

    for p in range(2):
        cols = pl.ds(p * hc, hc)
        w_piece(p).wait()
        with jax.named_scope(f"first{p}"):
            sbuf[0, :RB, cols] = jnp.dot(a[:RB], w[0, :, cols], preferred_element_type=f32).astype(bf)
        if p == 0:
            w_start(1)
            with jax.named_scope("barrier_wait"):
                pl.semaphore_wait(barrier, n_tp - 1)

            @pl.when(core == 0)
            def _():
                piece_send(0)
        else:
            @pl.when(core == 1)
            def _():
                piece_send(0)

            piece_send(1)
    for j in range(2, DEPTH):
        w_start(j)
    wait(w.at[1], w_sem.at[0])
    with jax.named_scope("far_product"):
        top_product(1)
    far_send(1, 0).start()

    @pl.loop(1, nch)
    def _(j):
        w_start(j + DEPTH - 1)
        w_wait(j)
        for p in range(2):
            with jax.named_scope("far_product"):
                top_product(2 * j + p)
            far_send(2 * j + p, 0).start()

    a_bot.start()
    r_copy.start()
    g_copy.start()
    a_bot.wait()
    r_copy.wait()
    g_copy.wait()

    @pl.loop(0, half)
    def _(i):
        with jax.named_scope("bot_product"):
            sbuf[i, RB:] = jnp.dot(a[RB:], w[i], preferred_element_type=f32).astype(bf)

    def near_loop(first, body):
        @pl.loop(0, nch // 2)
        def _(k):
            j = first + k

            @pl.when(j + DEPTH - 1 < 2 * nch)
            def _():
                w_start(j + DEPTH - 1)

            w_wait(j)
            for p in range(2):
                with jax.named_scope("near_product"):
                    body(2 * k + p, jnp.dot(a[...], w[2 * j + p], preferred_element_type=f32))

    def to_partner(c, x):
        sbuf[half + c] = x.astype(bf)
        pltpu.make_async_remote_copy(
            src_ref=sbuf.at[half + c], dst_ref=rbuf.at[0, c], send_sem=send_sem, recv_sem=part_sem,
            device_id=dev(partner), device_id_type=MESH).start()

    def keep(c, x):
        cols = pl.ds(pl.multiple_of(c * CN, CN), CN)
        own[c] = x + res[:, cols].astype(f32)

    near_loop(nch, to_partner)
    near_loop(nch + nch // 2, keep)
    wait(rbuf.at[0], part_sem)

    @pl.loop(0, nch)
    def _(c):
        own[c] = own[c] + rbuf[0, c].astype(f32)

    def issue(b, lo, hi):
        if 1 <= b < nrb:
            for c in range(lo, hi):
                far_send(2 * c, b).start()
                far_send(2 * c + 1, b).start()

    def add_chunk(b, c):
        cols = pl.ds(c * CN, CN)
        rs = block(b)
        h = own[c, rs, :] + (rbuf[1, c, rs, :].astype(f32) + rbuf[2, c, rs, :].astype(f32))
        hid_ref[rs, cols] = h.astype(bf)
        if b == last:
            last_ref[:, cols] = h
        else:
            own[c, rs, :] = h
        s = fold(h * h)
        sq[b] = s if c == 0 else sq[b] + s

    def stat_copy(b, k):
        return pltpu.make_async_remote_copy(
            src_ref=st_out.at[b], dst_ref=st_in.at[b, k - 1], send_sem=sst_sem,
            recv_sem=rst_sem.at[b], device_id=dev((me + k) % n_tp), device_id_type=MESH)

    def send_stats(b):
        with jax.named_scope(f"send_stats{b}"):
            t = jnp.sum(sq[b].T, axis=0, keepdims=True)
            st_out[b] = jnp.broadcast_to(t, (8, RB))
            for k in (2, 3, 1):
                stat_copy(b, k).start()

    def scale(b):
        with jax.named_scope(f"stat_wait{b}"):
            wait(st_in.at[b], rst_sem.at[b])
        t = st_out[b] + st_in[b, 0] + st_in[b, 1] + st_in[b, 2]
        return lax.rsqrt(t / d_model + EPS)

    def normalise(b):
        sq[b] = spread(scale(b))

        @pl.loop(0, nch)
        def _(c):
            for k in range(CN // LANES):
                cols = pl.ds(pl.multiple_of(c * CN + k * LANES, LANES), LANES)
                v = own[c, block(b), k * LANES:(k + 1) * LANES] * sq[b] * gain[:, cols]
                nrm_ref[block(b), cols] = v.astype(bf)

    for b in range(nrb):
        for n, (lo, hi) in enumerate(groups(b)):
            if b > 0 and n == 2:
                normalise(b - 1)
            with jax.named_scope(f"far_wait{b}_{n}"):
                wait(rbuf.at[pl.ds(1, 2), pl.ds(lo, hi - lo), block(b), :], far_sem.at[group_of(lo, b)])
            if n == 0:
                issue(b + 1, 0, quarter)
            for c in range(lo, hi):
                add_chunk(b, c)
        send_stats(b)
        issue(b + 1, quarter, nch)

    with jax.named_scope("drain"):
        wait(sbuf, send_sem)
    scale_ref[...] = scale(last)
    with jax.named_scope("drain2"):
        wait(st_in, sst_sem)


def finish_kernel(hid_ref, nrm_ref, last_ref, scale_ref, gain_ref, hid_hbm, nrm_hbm, buf, scale, sem):
    rows, d_local = hid_hbm.shape
    early = nrm_ref.shape[0]
    late = pl.ds(early, rows - early)
    copies = [
        pltpu.make_async_copy(hid_ref, hid_hbm, sem.at[0]),
        pltpu.make_async_copy(nrm_ref, nrm_hbm.at[pl.ds(0, early)], sem.at[1]),
    ]
    for c in copies:
        c.start()

    scale[...] = spread(scale_ref[...])

    @pl.loop(0, d_local // LANES)
    def _(j):
        cols = pl.ds(pl.multiple_of(j * LANES, LANES), LANES)
        buf[:, cols] = (last_ref[:, cols] * scale[...] * gain_ref[:, cols]).astype(jnp.bfloat16)

    copies.append(pltpu.make_async_copy(buf, nrm_hbm.at[late], sem.at[2]))
    copies[-1].start()
    for c in copies:
        c.wait()


def solution(mesh):
    n_tp = mesh.shape["tp"]

    def local_step(attn_blk, w_blk, resid_blk, gain_blk):
        rows, depth = attn_blk.shape
        d_local = resid_blk.shape[1]
        nch = d_local // CN
        nrb = rows // RB
        bf, f32 = jnp.bfloat16, jnp.float32
        dma = pltpu.SemaphoreType.DMA
        vmem = pl.BlockSpec(memory_space=pltpu.VMEM)
        hbm = pl.BlockSpec(memory_space=pl.ANY)
        parts = pl.pallas_call(
            functools.partial(main_kernel, n_tp),
            out_shape=(
                pltpu.VMEM((rows, d_local), bf),
                pltpu.VMEM((rows - RB, d_local), bf),
                pltpu.VMEM((RB, d_local), f32),
                pltpu.VMEM((8, RB), f32),
                pltpu.VMEM((1, d_local), f32),
            ),
            in_specs=[hbm] * 4,
            out_specs=(vmem,) * 5,
            scratch_shapes=[
                pltpu.VMEM((rows, depth), bf),
                pltpu.VMEM((4 * nch, depth, CN), bf),
                pltpu.VMEM((rows, d_local), bf),
                pltpu.VMEM((3 * nch, rows, CN), bf),
                pltpu.VMEM((nch, rows, CN), f32),
                pltpu.VMEM((3, nch, rows, CN), bf),
                pltpu.VMEM((nrb, RB, LANES), f32),
                pltpu.VMEM((nrb, 8, RB), f32),
                pltpu.VMEM((nrb, n_tp - 1, 8, RB), f32),
                dma((3,)), dma, dma((WSEM,)), dma, dma((2 * nrb + 2,)), dma, dma, dma((nrb,)),
            ],
            compiler_params=pltpu.CompilerParams(
                collective_id=0, has_side_effects=True, vmem_limit_bytes=54 * 1024 * 1024),
        )(attn_blk, w_blk, resid_blk, gain_blk.reshape(1, d_local))
        out = jax.ShapeDtypeStruct((rows, d_local), bf)
        return pl.pallas_call(
            finish_kernel,
            out_shape=(out, out),
            in_specs=[vmem] * 5,
            out_specs=(hbm, hbm),
            scratch_shapes=[pltpu.VMEM((RB, d_local), bf), pltpu.VMEM((RB, LANES), f32), dma((3,))],
            compiler_params=pltpu.CompilerParams(vmem_limit_bytes=4 * 1024 * 1024),
        )(*parts)

    return jax.shard_map(
        local_step,
        mesh=mesh,
        in_specs=(P("data", "tp"), P("tp", None), P("data", "tp"), P("tp")),
        out_specs=(P("data", "tp"), P("data", "tp")),
        check_vma=False,
    )
```
